32 devices in a mesh: section: 2 (over x), fsdp: 16 (over z, y, core).
Axes of the slice: x: 2, y: 2, z: 4, core: 2. Of those that a mesh axis runs over, the one named last changes fastest.
Arguments:
- hidden_in: bfloat16 [8, 16, 64, 1536], P(None, 'fsdp'), may hold values from -6 to 6
- norm_gain: float32 [2, 2, 1536], P(None, 'section'), may hold values from 0.25 to 1.75
- qkv_weight: bfloat16 [2, 2, 1536, 2048], P(None, 'section', 'fsdp'), may hold values from -0.15625 to 0.15625
- qkv_bias: float32 [2, 2, 2048], P(None, 'section'), may hold values from -30 to 30, as said below
- out_weight: bfloat16 [2, 2, 1536, 1536], P(None, 'section', 'fsdp'), may hold values from -0.15625 to 0.15625
Outputs:
- hidden_out: bfloat16 [8, 16, 64, 1536], P('section', 'fsdp')
The draws below stay inside these ranges and needn't reach their ends.
Inputs may be any that keep to these rules, and one draw needn't show every extreme that they name: `qkv_bias`: entries of the query, key and value biases.
All inputs are finite; a program needn't handle non-finite values.
Results may differ from the reference program's by a relative error of at most 0.035.
Values may be sent and summed in bfloat16 or wider, within the bound.
No kernel may reach another device: no remote copies, remote signals or barrier semaphores. Data moves between devices by JAX's collectives and lax.ppermute only.
A program may use at most 128 MiB of HBM per device.

```python
import math
import jax
import jax.numpy as jnp
from jax import lax

D = 1536
HEADS = 12
KV_HEADS = 2
HEAD_DIM = 128
LEN = 64
MICRO = 8
SPANS = 2
SEQS = 16
QKV = 2048
N_SECTION = 2


def draw_qkv_bias(key, part):
    bias_shape = (SPANS, N_SECTION, QKV)
    return jnp.clip(0.5 * jax.random.normal(key, bias_shape, jnp.float32), -3.0, 3.0)


def block_levels(key, extent, shards, least, top_value):
    def one(position, shards_of):
        heights = jax.random.uniform(jax.random.fold_in(jax.random.fold_in(key, 6), position), (shards_of,), jnp.float32, least / len(shards), top_value / len(shards))
        return jnp.repeat(jnp.exp(heights), extent[position] // shards_of).reshape((-1,) + (1,) * (len(extent) - position - 1))

    loudness = one(*shards[0])
    for cut in shards[1:]:
        loudness = loudness * one(*cut)
    return loudness


def scatter_about(stream_key, dims, deviation, most, split=(), kind=jnp.bfloat16):
    values = jax.random.normal(stream_key, dims, jnp.float32) * deviation
    if len(split) > 0:
        values = block_levels(stream_key, dims, split, -0.22, 0.18) * values
    return jnp.clip(values, min=-most, max=most).astype(kind)


def setup_inputs(seed: int = 0) -> dict:
    arg_keys = jax.random.split(jax.random.key(seed), 6)
    return {
        "hidden_in": scatter_about(arg_keys[0], (MICRO, SEQS, LEN, D), 1.0, 6.0, ((1, 16),)),
        "norm_gain": jnp.clip(1.0 + 0.15 * jax.random.normal(arg_keys[1], (SPANS, N_SECTION, D), jnp.float32), 0.25, 1.75),
        "qkv_weight": scatter_about(arg_keys[2], (SPANS, N_SECTION, D, QKV), D ** -0.5, 0.15625, ((1, 2), (2, 16))),
        "qkv_bias": draw_qkv_bias(jax.random.fold_in(arg_keys[5], 71), 0),
        "out_weight": scatter_about(arg_keys[4], (SPANS, N_SECTION, D, D), D ** -0.5, 0.15625, ((1, 2), (2, 16))),
    }


THETA = 1000000.0
EPS = 1.0

def rotate(tensor, cosine, sine_part):
    half_dim = tensor.shape[-1] // 2
    leading = tensor[..., :half_dim]
    second = tensor[..., half_dim:]
    return jnp.concatenate([leading * cosine - second * sine_part, second * cosine + leading * sine_part], axis=-1)

def attend_layer(hidden, gain, w_qkv, bias, w_out):
    rows, length, width = hidden.shape
    group_size = HEADS // KV_HEADS
    kv_width = KV_HEADS * HEAD_DIM
    wide = hidden.astype(jnp.float32)
    inv_rms = lax.rsqrt(lax.optimization_barrier(jnp.mean(wide * wide, axis=-1, keepdims=True)) + EPS)
    normed = (wide * inv_rms * gain).astype(jnp.bfloat16)
    projected = jnp.dot(normed.reshape(rows * length, width), w_qkv, preferred_element_type=jnp.float32) + bias
    projected = projected.reshape(rows, length, width + 2 * kv_width)
    queries = projected[..., :width].reshape(rows, length, KV_HEADS, group_size, HEAD_DIM)
    key_rows = projected[..., width:width + kv_width].reshape(rows, length, KV_HEADS, HEAD_DIM)
    value_rows = projected[..., width + kv_width:].astype(jnp.bfloat16).reshape(rows, length, KV_HEADS, HEAD_DIM)
    half_dim = HEAD_DIM // 2
    frequency = jnp.exp(jnp.arange(half_dim, dtype=jnp.float32) * (-2.0 * math.log(THETA) / HEAD_DIM))
    angles = jnp.arange(length, dtype=jnp.float32)[:, None] * frequency[None, :]
    cosine = jnp.cos(angles)
    sine_part = jnp.sin(angles)
    queries = rotate(queries, cosine[None, :, None, None, :], sine_part[None, :, None, None, :])
    key_rows = rotate(key_rows, cosine[None, :, None, :], sine_part[None, :, None, :])
    scores = jnp.einsum('rqkgd,rpkd->rkgqp', queries, key_rows, precision=lax.Precision.HIGHEST) / math.sqrt(HEAD_DIM)
    causal = jnp.arange(length)[:, None] >= jnp.arange(length)[None, :]
    scores = jnp.where(causal, scores, -1e+30)
    row_max = lax.optimization_barrier(jnp.max(scores, axis=-1, keepdims=True))
    weights = jnp.exp(scores - row_max)
    probability = (weights / lax.optimization_barrier(jnp.sum(weights, axis=-1, keepdims=True))).astype(jnp.bfloat16)
    context = jnp.einsum('rkgqp,rpkd->rqkgd', probability.astype(jnp.float32), value_rows.astype(jnp.float32), precision=lax.Precision.HIGHEST)
    context = context.reshape(rows, length, width).astype(jnp.bfloat16)
    update = jnp.dot(context.reshape(rows * length, width), w_out, preferred_element_type=jnp.float32)
    return (wide + update.reshape(rows, length, width)).astype(jnp.bfloat16)

def reference(hidden_in, norm_gain, qkv_weight, qkv_bias, out_weight):
    hidden = hidden_in
    for span_no in range(norm_gain.shape[0]):
        for section_no in range(norm_gain.shape[1]):

            def apply_layer(block_rows, span_no=span_no, section_no=section_no):
                return attend_layer(block_rows, norm_gain[span_no, section_no], qkv_weight[span_no, section_no], qkv_bias[span_no, section_no], out_weight[span_no, section_no])
            hidden = lax.map(apply_layer, hidden)
    return hidden
```

```python
import math

import jax
import jax.numpy as jnp
import numpy as np
from jax import lax
from jax.experimental import pallas as pl
from jax.experimental.pallas import tpu as pltpu
from jax.sharding import PartitionSpec as P

HEADS = 12
KV_HEADS = 2
HEAD_DIM = 128
THETA = 1000000.0
EPS = 1.0
LAG = 2
MIN_CHUNKS = 4


def ring_order(count):
    chips = list(range(0, count // 2, 2)) + list(range(1, count // 2, 2))[::-1]
    return [2 * chip + core for chip in chips for core in range(2)]


def ring_gather(shard, axis):
    count = lax.axis_size(axis)
    order = ring_order(count)
    right = [(order[i], order[(i + 1) % count]) for i in range(count)]
    left = [(b, a) for a, b in right]
    units = [shard]
    from_left = from_right = shard
    for step in range(count // 2):
        from_left = lax.ppermute(from_left, axis, right)
        units.append(from_left)
        if step < (count - 1) // 2:
            from_right = lax.ppermute(from_right, axis, left)
            units.append(from_right)
    return units


def unit_rows(count):
    order = ring_order(count)
    table = np.zeros((count, count), np.int32)
    for position, device in enumerate(order):
        row = [order[position]]
        for step in range(count // 2):
            row.append(order[(position - step - 1) % count])
            if step < (count - 1) // 2:
                row.append(order[(position + step + 1) % count])
        table[device] = row
    return table


def split(wide):
    high = wide.astype(jnp.bfloat16)
    low = (wide - high.astype(jnp.float32)).astype(jnp.bfloat16)
    return high, low


def layer_kernel(count, length, scal, own, arrived, gain, bias, cosine, sine, *rest):
    q_units, o_units = rest[:count], rest[count : 2 * count]
    out, w_qkv, w_out, x_in, proj, ctx, sem_x, sem_q, sem_o = rest[2 * count :]
    rows, width = x_in.shape
    part = q_units[0].shape[0]
    group = HEADS // KV_HEADS
    span = min(rows, 2 * length)
    kv_width = KV_HEADS * HEAD_DIM

    @pl.when(scal[0] == 1)
    def _():
        def place(units, target, sems, u):
            row = pl.multiple_of(scal[2 + u] * part, part)
            return pltpu.make_async_copy(units[u], target.at[pl.ds(row, part), :], sems.at[u])

        @pl.when(scal[1] == 1)
        def _():
            pltpu.make_async_copy(own, x_in, sem_x).start()

        @pl.when(scal[1] == 0)
        def _():
            pltpu.make_async_copy(arrived, x_in, sem_x).start()

        for u in range(count):
            place(q_units, w_qkv, sem_q, u).start()
        for u in range(count):
            place(o_units, w_out, sem_o, u).start()
        pltpu.make_async_copy(own, x_in, sem_x).wait()
        wide = x_in[...].astype(jnp.float32)
        inv_rms = lax.rsqrt(jnp.mean(wide * wide, axis=-1, keepdims=True) + EPS)
        normed = (wide * inv_rms * gain[...]).astype(jnp.bfloat16)
        for u in range(count):
            place(q_units, w_qkv, sem_q, u).wait()
        tile = 256
        for n in range(0, width + 2 * kv_width, tile):
            proj[:, n : n + tile] = (
                jnp.dot(normed, w_qkv[:, n : n + tile], preferred_element_type=jnp.float32)
                + bias[:, n : n + tile]
            )

        def rotate(head):
            return head * cosine[...] + pltpu.roll(head, HEAD_DIM // 2, 1) * sine[...]

        query_pos = lax.broadcasted_iota(jnp.int32, (span, span), 0)
        key_pos = lax.broadcasted_iota(jnp.int32, (span, span), 1)
        allowed = (query_pos >= key_pos) & (query_pos // length == key_pos // length)
        allowed = jnp.concatenate([allowed] * group, axis=0)
        for r in range(0, rows, span):
            for g in range(KV_HEADS):
                at = width + g * HEAD_DIM
                k_high, k_low = split(rotate(proj[r : r + span, at : at + HEAD_DIM]))
                keys = jnp.concatenate(
                    [
                        jnp.concatenate([k_high, k_high], axis=1),
                        jnp.concatenate([k_low, k_low], axis=1),
                    ],
                    axis=0,
                )
                heads = []
                for h in range(g * group, (g + 1) * group):
                    q_high, q_low = split(
                        rotate(proj[r : r + span, h * HEAD_DIM : (h + 1) * HEAD_DIM])
                    )
                    heads.append(jnp.concatenate([q_high, q_low], axis=1))
                queries = jnp.concatenate(heads, axis=0)
                both = lax.dot_general(
                    queries, keys, (((1,), (1,)), ((), ())), preferred_element_type=jnp.float32
                )
                scores = (both[:, :span] + both[:, span:]) * (1.0 / math.sqrt(HEAD_DIM))
                scores = jnp.where(allowed, scores, -1e30)
                row_max = jnp.max(scores, axis=-1, keepdims=True)
                weights = jnp.exp(scores - row_max)
                total = jnp.sum(weights, axis=-1, keepdims=True)
                probability = (weights / total).astype(jnp.bfloat16)
                at = width + kv_width + g * HEAD_DIM
                values = proj[r : r + span, at : at + HEAD_DIM].astype(jnp.bfloat16)
                mixed = jnp.dot(probability, values, preferred_element_type=jnp.float32)
                mixed = mixed.astype(jnp.bfloat16)
                for j in range(group):
                    at = (g * group + j) * HEAD_DIM
                    ctx[r : r + span, at : at + HEAD_DIM] = mixed[j * span : (j + 1) * span]
        for u in range(count):
            place(o_units, w_out, sem_o, u).wait()
        for n in range(0, width, tile):
            update = jnp.dot(ctx[...], w_out[:, n : n + tile], preferred_element_type=jnp.float32)
            out[:, n : n + tile] = (
                x_in[:, n : n + tile].astype(jnp.float32) + update
            ).astype(jnp.bfloat16)


def layer(scal, own, arrived, gain, bias, tables, q_units, o_units, length):
    count = len(q_units)
    rows, width = own.shape
    q_cols = q_units[0].shape[1]
    o_cols = o_units[0].shape[1]
    part = q_units[0].shape[0]
    vmem = pl.BlockSpec(memory_space=pltpu.VMEM)
    hbm = pl.BlockSpec(memory_space=pl.ANY)
    flops = 2 * rows * count * part * (q_cols + o_cols)

    def body(*refs):
        layer_kernel(count, length, *refs)

    return pl.pallas_call(
        body,
        out_shape=jax.ShapeDtypeStruct((rows, width), jnp.bfloat16),
        in_specs=[pl.BlockSpec(memory_space=pltpu.SMEM), hbm, hbm, vmem, vmem, vmem, vmem]
        + [hbm] * (2 * count),
        out_specs=vmem,
        scratch_shapes=[
            pltpu.VMEM((count * part, q_cols), jnp.bfloat16),
            pltpu.VMEM((count * part, o_cols), jnp.bfloat16),
            pltpu.VMEM((rows, width), jnp.bfloat16),
            pltpu.VMEM((rows, q_cols), jnp.float32),
            pltpu.VMEM((rows, width), jnp.bfloat16),
            pltpu.SemaphoreType.DMA(()),
            pltpu.SemaphoreType.DMA((count,)),
            pltpu.SemaphoreType.DMA((count,)),
        ],
        compiler_params=pltpu.CompilerParams(vmem_limit_bytes=24 << 20),
        cost_estimate=pl.CostEstimate(
            flops=flops, transcendentals=0, bytes_accessed=2 * count * part * (q_cols + o_cols)
        ),
        name="layer",
    )(scal, own, arrived, gain, bias, *tables, *q_units, *o_units)


def rope_tables(length, rows):
    half_dim = HEAD_DIM // 2
    frequency = jnp.exp(
        jnp.arange(half_dim, dtype=jnp.float32) * (-2.0 * math.log(THETA) / HEAD_DIM)
    )
    angles = jnp.arange(length, dtype=jnp.float32)[:, None] * frequency[None, :]
    cosine = jnp.cos(angles)
    sine = jnp.sin(angles)
    repeat = min(rows // length, 2)
    cosine = jnp.tile(jnp.concatenate([cosine, cosine], axis=1), (repeat, 1))
    sine = jnp.tile(jnp.concatenate([-sine, sine], axis=1), (repeat, 1))
    return cosine, sine


def per_device(hidden_in, norm_gain, qkv_weight, qkv_bias, out_weight):
    sections = lax.axis_size("section")
    my_section = lax.axis_index("section")
    count = lax.axis_size("fsdp")
    micro, local, length, width = hidden_in.shape
    spans = norm_gain.shape[0]
    chunks = max(sections, MIN_CHUNKS)
    owned = chunks // sections
    hidden = hidden_in.reshape(chunks, -1, width)
    rows = hidden.shape[1]
    tables = rope_tables(length, rows)
    order = jnp.asarray(unit_rows(count))[lax.axis_index("fsdp")]
    gathered = [
        (ring_gather(qkv_weight[c, 0], "fsdp"), ring_gather(out_weight[c, 0], "fsdp"))
        for c in range(spans)
    ]
    entering = [hidden[j] for j in range(chunks)]
    finished = [None] * chunks
    received = [None] * chunks
    for c in range(spans):
        ticks = chunks + LAG * (sections - 1)
        last = c == spans - 1
        moved = [None] * ticks
        leaving = [None] * chunks
        for t in range(ticks):
            item = t - LAG * my_section
            active = (item >= 0) & (item < chunks)
            own = entering[min(t, chunks - 1)]
            arrived = moved[t - LAG] if t >= LAG else own
            scal = jnp.concatenate(
                [jnp.stack([active, my_section == 0]).astype(jnp.int32), order]
            )
            out = layer(
                scal,
                own,
                arrived,
                norm_gain[c],
                qkv_bias[c],
                tables,
                *gathered[c],
                length,
            )
            senders = [
                i for i in range(sections) if 0 <= t - LAG * i < chunks and i < sections - 1
            ]
            route = [(i, i + 1) for i in senders]
            done = t - LAG * (sections - 1)
            if 0 <= done < chunks and not last:
                route.append((sections - 1, 0))
            if route:
                moved[t] = lax.ppermute(out, "section", route)
            if 0 <= done < chunks:
                if not last:
                    leaving[done] = moved[t]
                else:
                    finished[done] = out
                    owner = done // owned
                    if owner != sections - 1:
                        received[done] = lax.ppermute(out, "section", [(sections - 1, owner)])
        entering = leaving
    results = []
    for j in range(owned):
        piece = finished[(sections - 1) * owned + j]
        for s in range(sections - 1):
            piece = jnp.where(my_section == s, received[s * owned + j], piece)
        results.append(piece)
    result = jnp.stack(results)
    return result.reshape(micro // sections, local, length, width)


def solution(mesh):
    in_specs = (
        P(None, "fsdp", None, None),
        P(None, "section", None),
        P(None, "section", "fsdp", None),
        P(None, "section", None),
        P(None, "section", "fsdp", None),
    )
    out_specs = P("section", "fsdp", None, None)
    return jax.shard_map(
        per_device, mesh=mesh, in_specs=in_specs, out_specs=out_specs, check_vma=False
    )
```
